32 devices in a mesh: ey: 4 (over z), ex: 8 (over y, x, core).
Axes of the slice: x: 2, y: 2, z: 4, core: 2. Of those that a mesh axis runs over, the one named last changes fastest.
Arguments:
- x: bfloat16 [2048, 2048], P(('ey', 'ex'))
- kv_k: bfloat16 [2048, 256, 1, 128], P(('ey', 'ex'))
- kv_v: bfloat16 [2048, 256, 1, 128], P(('ey', 'ex'))
- lens: int32 [2048], P(('ey', 'ex'))
- topk_idx: int32 [2048, 6], P(('ey', 'ex'))
- gates: float32 [2048, 6], P(('ey', 'ex'))
- ln1: bfloat16 [2048], replicated
- ln2: bfloat16 [2048], replicated
- wq: bfloat16 [2048, 2048], replicated
- wo: bfloat16 [2048, 2048], replicated
- ws1: bfloat16 [2048, 1408], replicated
- ws3: bfloat16 [2048, 1408], replicated
- ws2: bfloat16 [1408, 2048], replicated
- w1: bfloat16 [64, 2048, 1408], P(('ey', 'ex'))
- w3: bfloat16 [64, 2048, 1408], P(('ey', 'ex'))
- w2: bfloat16 [64, 1408, 2048], P(('ey', 'ex'))
Outputs:
- output: bfloat16 [2048, 2048], P(('ey', 'ex'))
All inputs are finite; a program needn't handle non-finite values.
Results may differ from the reference program's by a relative error of at most 0.0123182.
Values are sent between devices in bfloat16 or wider.
A program may use at most 1 GiB of HBM per device.

```python
import jax
import jax.numpy as jnp
from jax import lax

EY = 4
EX = 8
TOKENS = 64
LEN = 256
D = 2048
HEADS = 16
KV_HEADS = 1
HEAD = 128
FF = 1408
EXPERTS = 64
TOP = 6
ROWS_MAX = 2
CAP = 12
EPS = 1e-6
GATE_SCALE = 2.5

NDEV = EY * EX
NT = NDEV * TOKENS
EROW = EXPERTS // EY
NSLOT = EXPERTS * NDEV * CAP


def _normal(key, shape, scale):
    return (scale * jax.random.normal(key, shape, jnp.float32)).astype(jnp.bfloat16)


def _stack(key, n, shape, scale):
    return lax.map(lambda k: _normal(k, shape, scale), jax.random.split(key, n))


def _route(key):
    place_key, token_key = jax.random.split(key)
    places = jax.random.permutation(place_key, jnp.arange(EXPERTS, dtype=jnp.int32))
    half_count = EXPERTS // 2
    upper_span = EXPERTS - 1 - half_count
    offset = places - half_count
    square = offset * offset
    weight = jnp.where(offset < 0, 100 - (square * 78) // (half_count * half_count), 100 + (square * 350) // (upper_span * upper_span)).astype(jnp.uint32)
    row_of = jnp.arange(EXPERTS) // EROW

    def pick_one(one_key):
        order_key, count_key, noise_key = jax.random.split(one_key, 3)
        row_order = jax.random.permutation(order_key, EY)
        rows_used = jax.random.randint(count_key, (), 1, ROWS_MAX + 1)
        allowed = jnp.zeros((EY,), jnp.int32).at[row_order].set((jnp.arange(EY) < rows_used).astype(jnp.int32))
        noise_bits = jax.random.bits(noise_key, (EXPERTS,), jnp.uint32) >> 10
        waiting = jnp.where(allowed[row_of] > 0, noise_bits * weight, jnp.uint32(0xFFFFFFFF))
        return jnp.argsort(waiting)[:TOP]
    return jax.vmap(pick_one)(jax.random.split(token_key, NT)).astype(jnp.int32)


def setup_inputs(seed: int = 0) -> dict:
    ks = jax.random.split(jax.random.key(seed), 16)
    kd = jax.random.split(jax.random.fold_in(jax.random.key(seed), 7), 3)
    hd = HEADS * HEAD
    full = jax.random.uniform(kd[0], (NT,), jnp.float32) < 0.3
    short = jax.random.randint(kd[1], (NT,), 1, LEN // 8 + 1, jnp.int32)
    return {
        'x': _normal(ks[0], (NT, D), 1.0),
        'kv_k': _stack(ks[1], NT, (LEN, KV_HEADS, HEAD), 2.0),
        'kv_v': _stack(ks[2], NT, (LEN, KV_HEADS, HEAD), 1.0),
        'lens': jnp.where(full, LEN, short).astype(jnp.int32),
        'topk_idx': _route(kd[2]),
        'gates': GATE_SCALE * jax.nn.softmax(0.5 * jax.random.normal(ks[5], (NT, TOP), jnp.float32), axis=-1),
        'ln1': (1.0 + 0.1 * jax.random.normal(ks[6], (D,), jnp.float32)).astype(jnp.bfloat16),
        'ln2': (1.0 + 0.1 * jax.random.normal(ks[7], (D,), jnp.float32)).astype(jnp.bfloat16),
        'wq': _normal(ks[8], (D, hd), D ** -0.5),
        'wo': _normal(ks[9], (hd, D), hd ** -0.5),
        'ws1': _normal(ks[10], (D, FF), D ** -0.5),
        'ws3': _normal(ks[11], (D, FF), D ** -0.5),
        'ws2': _normal(ks[12], (FF, D), FF ** -0.5),
        'w1': _stack(ks[13], EXPERTS, (D, FF), D ** -0.5),
        'w3': _stack(ks[14], EXPERTS, (D, FF), D ** -0.5),
        'w2': _stack(ks[15], EXPERTS, (FF, D), FF ** -0.5),
    }


def _rms(v, w):
    v = v.astype(jnp.float32)
    r = lax.rsqrt(jnp.mean(v * v, axis=-1, keepdims=True) + EPS)
    return (v * r * w.astype(jnp.float32)).astype(jnp.bfloat16)


def _ffn(u, w1, w3, w2):
    g = jnp.dot(u, w1, preferred_element_type=jnp.float32)
    v = jnp.dot(u, w3, preferred_element_type=jnp.float32)
    z = (jax.nn.silu(g) * v).astype(jnp.bfloat16)
    return jnp.dot(z, w2, preferred_element_type=jnp.float32).astype(jnp.bfloat16)


def _attn(x, kk, vv, lens, ln1, wq, wo):
    b = x.shape[0]
    a = _rms(x, ln1)
    q = jnp.dot(a, wq, preferred_element_type=jnp.float32).astype(jnp.bfloat16)
    q = q.reshape(b, KV_HEADS, HEADS // KV_HEADS, HEAD).astype(jnp.float32)
    s = jnp.einsum('bkgd,blkd->bkgl', q, kk.astype(jnp.float32)) * HEAD ** -0.5
    valid = jnp.arange(LEN)[None, :] < lens[:, None]
    s = jnp.where(valid[:, None, None, :], s, -jnp.inf)
    p = jax.nn.softmax(s, axis=-1).astype(jnp.bfloat16).astype(jnp.float32)
    o = jnp.einsum('bkgl,blkd->bkgd', p, vv.astype(jnp.float32)).astype(jnp.bfloat16)
    attn = jnp.dot(o.reshape(b, HEADS * HEAD), wo, preferred_element_type=jnp.float32)
    return (x.astype(jnp.float32) + attn).astype(jnp.bfloat16)


def _slots(topk_idx, gates):
    chosen = (topk_idx[:, :, None] == jnp.arange(EXPERTS)[None, None, :]).any(axis=1).astype(jnp.int32)
    chosen = chosen.reshape(NDEV, TOKENS, EXPERTS)
    before = (jnp.cumsum(chosen, axis=1) - chosen).reshape(NT, EXPERTS)
    rank = jnp.take_along_axis(before, topk_idx, axis=1)
    src = (jnp.arange(NT, dtype=jnp.int32) // TOKENS)[:, None]
    pos = jnp.where(rank < CAP, (topk_idx * NDEV + src) * CAP + rank, NSLOT).reshape(-1)
    tok = jnp.broadcast_to(jnp.arange(NT, dtype=jnp.int32)[:, None], (NT, TOP)).reshape(-1)
    slot_tok = jnp.full((NSLOT,), NT, jnp.int32).at[pos].set(tok, mode='drop')
    slot_gate = jnp.zeros((NSLOT,), jnp.float32).at[pos].set(gates.reshape(-1), mode='drop')
    return slot_tok.reshape(EXPERTS, NDEV * CAP), slot_gate.reshape(EXPERTS, NDEV * CAP)


def reference(x, kv_k, kv_v, lens, topk_idx, gates, ln1, ln2, wq, wo, ws1, ws3, ws2, w1, w3, w2):
    per_dev = lambda a: a.reshape((NDEV, TOKENS) + a.shape[1:])
    h = lax.map(lambda t: _attn(t[0], t[1], t[2], t[3], ln1, wq, wo),
                (per_dev(x), per_dev(kv_k), per_dev(kv_v), per_dev(lens))).reshape(NT, D)
    u = _rms(h, ln2)
    slot_tok, slot_gate = _slots(topk_idx, gates)
    u_pad = jnp.concatenate([u, jnp.zeros((1, D), jnp.bfloat16)], axis=0)

    def expert(acc, xs):
        tok, gate, a1, a3, a2 = xs
        e = _ffn(u_pad[tok], a1, a3, a2)
        return acc.at[tok].add(gate[:, None] * e.astype(jnp.float32)), None

    routed, _ = lax.scan(expert, jnp.zeros((NT + 1, D), jnp.float32), (slot_tok, slot_gate, w1, w3, w2))
    y = h.astype(jnp.float32) + _ffn(u, ws1, ws3, ws2).astype(jnp.float32) + routed[:NT]
    return y.astype(jnp.bfloat16)
```

```python
import functools

import jax
import jax.numpy as jnp
from jax import lax
from jax.experimental import pallas as pl
from jax.experimental.pallas import tpu as pltpu
from jax.sharding import PartitionSpec as P

EPS = 1e-6
BF = jnp.bfloat16
F32 = jnp.float32
MESH = pl.DeviceIdType.MESH
META = 128
VMEM = pltpu.VMEM
ANY = pl.ANY


def _dot(a, b):
    return jnp.dot(a, b, preferred_element_type=F32)


def _dot_nt(a, b):
    return lax.dot_general(a, b, (((1,), (1,)), ((), ())), preferred_element_type=F32)


def _rms(v, w):
    v = v.astype(F32)
    r = lax.rsqrt(jnp.mean(v * v, axis=-1, keepdims=True) + EPS)
    return (v * r * w.astype(F32)).astype(BF)


def _split3(v):
    p1 = v.astype(BF)
    v = v - p1.astype(F32)
    p2 = v.astype(BF)
    p3 = (v - p2.astype(F32)).astype(BF)
    return p1, p2, p3


def _attn_kernel(nrow, n_exp, C, cap, lens, x, topk, gates, ln1, ln2, kk, vv, wq, wo,
                 h_out, u_out, xc_out, back_out,
                 wqv, wov, kv, vvv, qs, os, sw, so, sk, sv):
    b, d = x.shape
    l, dh = kk.shape[1], kk.shape[2]
    nh = wq.shape[1] // dh
    nw = sw.shape[0]
    wc = d // nw
    nk = sk.shape[0]
    tk = b // nk
    nt = topk.shape[0]

    def cq(i):
        return pltpu.make_async_copy(wq.at[:, pl.ds(i * wc, wc)], wqv.at[i], sw.at[i])

    def co(i):
        return pltpu.make_async_copy(wo.at[:, pl.ds(i * wc, wc)], wov.at[i], so.at[i])

    def ck(i):
        return pltpu.make_async_copy(kk.at[pl.ds(i * tk, tk)], kv.at[pl.ds(i * tk, tk)], sk.at[i])

    def cv(i):
        return pltpu.make_async_copy(vv.at[pl.ds(i * tk, tk)], vvv.at[pl.ds(i * tk, tk)], sv.at[i])

    for i in range(nw):
        cq(i).start()
    for i in range(nk):
        ck(i).start()
        cv(i).start()
    for i in range(nw):
        co(i).start()

    eio = lax.broadcasted_iota(jnp.int32, (n_exp, b), 0)
    ch = jnp.zeros((n_exp, b), F32)
    gt = jnp.zeros((n_exp, b), F32)
    for j in range(nt):
        hit = eio == topk[j:j + 1, :]
        ch = jnp.where(hit, 1.0, ch)
        gt = jnp.where(hit, gates[j:j + 1, :], gt)
    upper = (lax.broadcasted_iota(jnp.int32, (b, b), 0) < lax.broadcasted_iota(jnp.int32, (b, b), 1))
    upper = jnp.where(upper, 1.0, 0.0).astype(BF)
    rank = _dot(ch.astype(BF), upper)
    kept = (ch > 0) & (rank < cap)
    kp1 = jnp.where(kept, rank + 1.0, 0.0)
    g1, g2, g3 = _split3(jnp.where(kept, gt, 0.0))
    er = n_exp // nrow
    sels, metas = [], []
    cio = lax.broadcasted_iota(jnp.int32, (C, b), 0).astype(F32)
    for r in range(nrow):
        sl = slice(r * er, (r + 1) * er)
        need = jnp.max(jnp.where(kept[sl], 1.0, 0.0), axis=0, keepdims=True)
        need8 = jnp.broadcast_to(need, (8, b))
        cpos = _dot(need8.astype(BF), upper)[0:1]
        sel = jnp.where((cio == cpos) & (need > 0), 1.0, 0.0).astype(BF)
        sels.append(sel)
        m = jnp.concatenate([kp1[sl], g1[sl].astype(F32), g2[sl].astype(F32), g3[sl].astype(F32),
                             jnp.zeros((META - 4 * er, b), F32)], axis=0).astype(BF)
        metas.append(_dot_nt(sel, m).astype(BF))
    eye = (lax.broadcasted_iota(jnp.int32, (b, b), 0) == lax.broadcasted_iota(jnp.int32, (b, b), 1))
    eye = jnp.where(eye, 1.0, 0.0).astype(BF)
    selall = jnp.concatenate(sels, axis=0)
    back_out[...] = _dot_nt(eye, selall).astype(BF)

    a = _rms(x[...], ln1[...])
    hc = wc // dh
    for i in range(nw):
        cq(i).wait()
        q = _dot(a, wqv[i]).astype(BF).astype(F32)
        for j in range(hc):
            qs[:, i * hc + j, :] = q[:, j * dh:(j + 1) * dh]

    scale = dh ** -0.5
    lio = lax.broadcasted_iota(jnp.int32, (nh, l), 1)
    un = 8

    def group(g, _):
        for i in range(nk):
            @pl.when(g * un == i * tk)
            def _():
                ck(i).wait()
                cv(i).wait()
        ts = [g * un + j for j in range(un)]
        ss = [_dot_nt(qs[t].astype(BF), kv[t]) for t in ts]
        ps = []
        for t, s in zip(ts, ss):
            s = jnp.where(lio < lens[t], s * scale, -jnp.inf)
            p = jnp.exp(s - jnp.max(s, axis=-1, keepdims=True))
            ps.append((p * (1.0 / jnp.sum(p, axis=-1, keepdims=True))).astype(BF))
        for t, p in zip(ts, ps):
            os[t] = _dot(p, vvv[t])
        return 0

    lax.fori_loop(0, b // un, group, 0)
    o = jnp.concatenate([os[:, j, :].astype(BF) for j in range(nh)], axis=1)
    hs = []
    for i in range(nw):
        co(i).wait()
        hs.append((x[:, i * wc:(i + 1) * wc].astype(F32) + _dot(o, wov[i])).astype(BF))
    h = jnp.concatenate(hs, axis=1)
    h_out[...] = h
    u = _rms(h, ln2[...])
    u_out[...] = u
    xall = _dot(selall, u).astype(BF)
    for r in range(nrow):
        xc_out[r, :, :d] = xall[r * C:(r + 1) * C]
        xc_out[r, :, d:] = metas[r]


def _attention(x, kk, vv, lens, topk_t, gates_t, ln1, ln2, wq, wo, nrow, n_exp, C, cap):
    b, d = x.shape
    _, l, _, dh = kk.shape
    kk, vv = kk.reshape(b, l, dh), vv.reshape(b, l, dh)
    nw, nk = 4, 4
    nh = wq.shape[1] // dh
    vm = pl.BlockSpec(memory_space=VMEM)
    an = pl.BlockSpec(memory_space=ANY)
    return pl.pallas_call(
        functools.partial(_attn_kernel, nrow, n_exp, C, cap),
        out_shape=[jax.ShapeDtypeStruct((b, d), BF), jax.ShapeDtypeStruct((b, d), BF),
                   jax.ShapeDtypeStruct((nrow, C, d + META), BF), jax.ShapeDtypeStruct((b, nrow * C), BF)],
        in_specs=[pl.BlockSpec(memory_space=pltpu.SMEM)] + [vm] * 5 + [an] * 4,
        out_specs=[vm] * 4,
        scratch_shapes=[
            pltpu.VMEM((nw, d, d // nw), BF), pltpu.VMEM((nw, d, d // nw), BF),
            pltpu.VMEM((b, l, dh), BF), pltpu.VMEM((b, l, dh), BF),
            pltpu.VMEM((b, nh, dh), F32), pltpu.VMEM((b, nh, dh), F32),
            pltpu.SemaphoreType.DMA((nw,)), pltpu.SemaphoreType.DMA((nw,)),
            pltpu.SemaphoreType.DMA((nk,)), pltpu.SemaphoreType.DMA((nk,)),
        ],
        name='attention',
        compiler_params=pltpu.CompilerParams(vmem_limit_bytes=56 * 2 ** 20),
    )(lens, x, topk_t, gates_t, ln1.reshape(1, d), ln2.reshape(1, d), kk, vv, wq, wo)


def _xor(a, b, bits):
    r = 0
    for i in range(bits):
        m = 2 ** i
        p, q = (a // m) % 2, (b // m) % 2
        r = r + m * ((p + q) % 2)
    return r


def _moe_kernel(ney, nex, C, cap, nj, fb,
                xc, h, u, back, ws1, ws3, ws2, w1, w3, w2, y,
                T, w1v, w3v, w2v, sa, sb, xin, act, O, R, PS, Q, G, acc, shr,
                s_loc, zs, zr, xs, xr, ys, yr, ds_, dr, ps, pr, s_w, s_w2, s_sa, s_sb, r1s, r1r, r2s, r2r):
    d = u.shape[1]
    edev, _, ff = w1.shape
    erow = edev * nex
    z = lax.axis_index('ey')
    e = lax.axis_index('ex')
    core, x, yy = e % 2, (e // 2) % 2, e // 4
    xn = yy * 4 + (1 - x) * 2 + core
    yn = (1 - yy) * 4 + x * 2 + core
    dg = (1 - yy) * 4 + (1 - x) * 2 + core
    pt = yy * 4 + x * 2 + (1 - core)
    H = C // 2

    def zx(i):
        return _xor(z, i, 2)

    def rcopy(src, dst, ss, rs, dev):
        return pltpu.make_async_remote_copy(src_ref=src, dst_ref=dst, send_sem=ss, recv_sem=rs,
                                            device_id=dev, device_id_type=MESH)

    ka = sa.shape[2]
    kb = sb.shape[1]
    na, nb = d // ka, ff // kb

    def c_a(i, slot):
        return [pltpu.make_async_copy(w.at[pl.ds(i * ka, ka)], sa.at[slot, m], s_sa.at[slot, m])
                for m, w in enumerate((ws1, ws3))]

    def c_b(i, slot):
        return pltpu.make_async_copy(ws2.at[pl.ds(i * kb, kb)], sb.at[slot], s_sb.at[slot])

    def c_w(m, k):
        src, dst = ((w1, w1v), (w3, w3v))[m]
        return pltpu.make_async_copy(src.at[k], dst.at[k], s_w.at[m, k])

    jc = d // nj

    def c_w2(j, slot):
        return pltpu.make_async_copy(w2.at[:, :, pl.ds(pl.multiple_of(j * jc, jc), jc)], w2v.at[slot], s_w2.at[slot])

    loc = pltpu.make_async_copy(xc.at[z], T.at[e, z], s_loc)
    loc.start()
    for i in range(2):
        for c in c_a(i, i):
            c.start()
    c_b(0, 0).start()
    c_b(1, 1).start()

    bar = pltpu.get_barrier_semaphore()
    peers = [(zx(i), e) for i in range(1, ney)] + [(z, _xor(e, q, 3)) for q in range(1, nex)]
    for dev in peers:
        pl.semaphore_signal(bar, inc=1, device_id=dev, device_id_type=MESH)
    pl.semaphore_wait(bar, len(peers))

    zc = [None] + [rcopy(xc.at[zx(i)], T.at[e, z], zs.at[i], zr.at[i], (zx(i), e)) for i in range(1, ney)]
    zw = [None] + [rcopy(xc.at[z], T.at[e, zx(i)], zs.at[i], zr.at[i], (zx(i), e)) for i in range(1, ney)]
    for i in range(1, ney):
        zc[i].start()
    for m in range(2):
        for k in range(edev):
            c_w(m, k).start()
    c_w2(0, 0).start()
    c_w2(1, 1).start()

    def half(c, s, hf):
        return T.at[c, s, pl.ds(hf * H, H)]

    def fwd(c, s, hf, ssem, rsem, dst):
        return rcopy(half(c, s, hf), half(c, s, hf), ssem, rsem, (z, dst))

    def to_x(i, hf):
        return fwd(e, zx(i), hf, xs.at[i, hf], xr.at[i, hf], xn)

    def to_y(i, hf):
        return fwd(e, zx(i), hf, ys.at[i, hf], yr.at[i, hf], yn)

    def to_d(i, hf):
        return fwd((xn, yn)[hf], zx(i), hf, ds_.at[i, hf], dr.at[i, hf], (yn, xn)[hf])

    def to_p(i, k):
        blk = T.at[(e, xn, yn, dg)[k], zx(i)]
        return rcopy(blk, blk, ps.at[i, k], pr.at[i, k], (z, pt))

    def stage1(i):
        if i == 0:
            loc.wait()
        else:
            zw[i].wait_recv()
        for hf in (0, 1):
            to_x(i, hf).start()
            to_y(i, 1 - hf).start()
        to_p(i, 0).start()

    def stage2(i):
        to_x(i, 0).wait_recv()
        to_d(i, 0).start()
        to_y(i, 1).wait_recv()
        to_d(i, 1).start()
        to_x(i, 1).wait_recv()
        to_p(i, 1).start()
        to_y(i, 0).wait_recv()
        to_p(i, 2).start()

    def stage3(i):
        to_d(i, 0).wait_recv()
        to_d(i, 1).wait_recv()
        to_p(i, 3).start()

    def shared_a():
        acc[...] = jnp.zeros_like(acc)

        def body(i, _):
            slot = i % 2
            for c in c_a(i, slot):
                c.wait()
            uc = u[:, pl.ds(pl.multiple_of(i * ka, ka), ka)]
            acc[0] += _dot(uc, sa[slot, 0])
            acc[1] += _dot(uc, sa[slot, 1])

            @pl.when(i + 2 < na)
            def _():
                for c in c_a(i + 2, slot):
                    c.start()
            return 0
        lax.fori_loop(0, na, body, 0)

    def shared_b():
        shr[...] = jnp.zeros_like(shr)
        zz = (jax.nn.silu(acc[0]) * acc[1]).astype(BF)
        for i in range(nb):
            slot = i % 2
            c_b(i, slot).wait()
            shr[...] += _dot(zz[:, i * kb:(i + 1) * kb], sb[slot])
            if i + 2 < nb:
                c_b(i + 2, slot).start()
        shr[...] = shr[...].astype(BF).astype(F32)

    def combine_matrix():
        M = T[e, :, :, d:].reshape(ney * C, META)
        n = erow * ney * cap
        ln = lax.broadcasted_iota(jnp.int32, (META, n), 1)
        er = lax.broadcasted_iota(jnp.int32, (META, n), 0)
        sp = ln // (ney * cap)
        ex = [jnp.where(er == sp + m * erow, 1.0, 0.0).astype(BF) for m in range(4)]
        k1 = _dot(M, ex[0])
        srow = lax.broadcasted_iota(jnp.int32, (ney * C, n), 0) // C
        pos = lax.broadcasted_iota(jnp.int32, (ney * C, n), 1) % (ney * cap)
        hit = (k1 > 0) & ((k1 + (srow * cap - 1).astype(F32)) == pos.astype(F32))
        for m in range(3):
            G[m] = jnp.where(hit, _dot(M, ex[m + 1]), 0.0).astype(BF)

    def gather(c, _):
        M = T[c, :, :, d:].reshape(ney * C, META)
        sel = (lax.broadcasted_iota(jnp.int32, (16, META), 1)
               == lax.broadcasted_iota(jnp.int32, (16, META), 0) + edev * e)
        sel = jnp.where(sel, 1.0, 0.0).astype(BF)
        V = _dot_nt(sel, M)
        rows = ney * cap
        s = lax.broadcasted_iota(jnp.int32, (1, ney * C), 1) // C
        pos = lax.broadcasted_iota(jnp.int32, (rows, ney * C), 0).astype(F32)
        X = T[c, :, :, :d].reshape(ney * C, d)
        for k in range(edev):
            v = V[k:k + 1]
            tgt = jnp.where(v > 0, v + (s * cap - 1).astype(F32), -1.0)
            xin[k, c] = _dot(jnp.where(pos == tgt, 1.0, 0.0).astype(BF), X).astype(BF)
        return 0

    stage1(0)
    shared_a()
    stage1(1)
    stage2(0)
    shared_b()
    stage1(2)
    stage2(1)
    stage3(0)
    stage1(3)
    combine_matrix()
    stage2(2)
    stage3(1)
    stage2(3)
    stage3(2)
    stage3(3)
    for i in range(ney):
        for k in range(4):
            to_p(i, k).wait_recv()
    lax.fori_loop(0, nex, gather, 0)

    rows = nex * ney * cap
    for k in range(edev):
        c_w(0, k).wait()
        c_w(1, k).wait()

        def ffn(f0, n):
            xk = xin[k].reshape(rows, d)
            g = _dot(xk, w1v[k, :, pl.ds(f0, n)])
            v = _dot(xk, w3v[k, :, pl.ds(f0, n)])
            act[k, :, pl.ds(f0, n)] = (jax.nn.silu(g) * v).astype(BF)

        def body(f, _):
            ffn(pl.multiple_of(f * fb, fb), fb)
            return 0
        lax.fori_loop(0, ff // fb, body, 0)
        if ff % fb:
            ffn(ff - ff % fb, ff % fb)

    slots = edev * ney * cap

    def r1(j, q):
        c = _xor(e, q, 3)
        return rcopy(O.at[j % 2, c], R.at[j, e], r1s.at[j % 2, q], r1r.at[j, q], (z, c))

    def r1w(j, q):
        c = _xor(e, q, 3)
        return rcopy(O.at[j % 2, c], R.at[j, c], r1s.at[j % 2, q], r1r.at[j, q], (z, c))

    def r2(j, i):
        s = zx(i)
        return rcopy(PS.at[j % 2, s], Q.at[j, z], r2s.at[j % 2, i], r2r.at[j, i], (s, e))

    def r2w(j, i):
        s = zx(i)
        return rcopy(PS.at[j % 2, s], Q.at[j, s], r2s.at[j % 2, i], r2r.at[j, i], (s, e))

    def step(j, _):
        @pl.when(j < nj)
        def _():
            c_w2(j, j % 2).wait()

            @pl.when(j >= 2)
            def _():
                for q in range(1, nex):
                    r1(j, q).wait_send()
            for k in range(edev):
                o = _dot(act[k], w2v[j % 2, k]).astype(BF)
                O[j % 2, :, k * ney * cap:(k + 1) * ney * cap, :] = o.reshape(nex, ney * cap, jc)

            @pl.when(j + 2 < nj)
            def _():
                c_w2(j + 2, j % 2).start()
            R[j, e] = O[j % 2, e]
            for q in range(1, nex):
                r1(j, q).start()

        @pl.when((j >= 1) & (j < nj + 1))
        def _():
            jj = j - 1

            @pl.when(jj >= 2)
            def _():
                for i in range(1, ney):
                    r2(jj, i).wait_send()
            for q in range(1, nex):
                r1w(jj, q).wait_recv()
            Rj = R[jj].reshape(nex * slots, jc)
            p = _dot(G[0], Rj) + _dot(G[1], Rj) + _dot(G[2], Rj)
            PS[jj % 2] = p.reshape(ney, C, jc)
            Q[jj, z] = PS[jj % 2, z]
            for i in range(1, ney):
                r2(jj, i).start()

        @pl.when(j >= 2)
        def _():
            jj = j - 2
            for i in range(1, ney):
                r2w(jj, i).wait_recv()
            q1, q2, q3 = _split3(Q[jj].reshape(ney * C, jc))
            bk = back[...]
            routed = _dot(bk, q1) + _dot(bk, q2) + _dot(bk, q3)
            cols = pl.ds(pl.multiple_of(jj * jc, jc), jc)
            y[:, cols] = (h[:, cols].astype(F32) + shr[:, cols] + routed).astype(BF)
        return 0

    lax.fori_loop(0, nj + 2, step, 0)

    for i in range(1, ney):
        zc[i].wait_send()
    for i in range(ney):
        for hf in (0, 1):
            to_x(i, hf).wait_send()
            to_y(i, hf).wait_send()
            to_d(i, hf).wait_send()
        for k in range(4):
            to_p(i, k).wait_send()
    for j in (nj - 2, nj - 1):
        for q in range(1, nex):
            r1(j, q).wait_send()
        for i in range(1, ney):
            r2(j, i).wait_send()


def _moe(xc, h, u, back, ws1, ws3, ws2, w1, w3, w2, ney, nex, C, cap):
    b, d = u.shape
    edev, _, ff = w1.shape
    nj, fb = 4, 256
    jc = d // nj
    rows = ney * cap
    vm = pl.BlockSpec(memory_space=VMEM)
    an = pl.BlockSpec(memory_space=ANY)
    DMA = pltpu.SemaphoreType.DMA
    ka, kb = 128, 176
    return pl.pallas_call(
        functools.partial(_moe_kernel, ney, nex, C, cap, nj, fb),
        out_shape=jax.ShapeDtypeStruct((b, d), BF),
        in_specs=[an, vm, vm, vm] + [an] * 6,
        out_specs=vm,
        scratch_shapes=[
            pltpu.VMEM((nex, ney, C, d + META), BF),
            pltpu.VMEM((edev, d, ff), BF), pltpu.VMEM((edev, d, ff), BF),
            pltpu.VMEM((2, edev, ff, jc), BF),
            pltpu.VMEM((2, 2, ka, ff), BF), pltpu.VMEM((2, kb, d), BF),
            pltpu.VMEM((edev, nex, rows, d), BF),
            pltpu.VMEM((edev, nex * rows, ff), BF),
            pltpu.VMEM((2, nex, edev * rows, jc), BF),
            pltpu.VMEM((nj, nex, edev * rows, jc), BF),
            pltpu.VMEM((2, ney, C, jc), F32),
            pltpu.VMEM((nj, ney, C, jc), F32),
            pltpu.VMEM((3, ney * C, nex * edev * rows), BF),
            pltpu.VMEM((2, b, ff), F32),
            pltpu.VMEM((b, d), F32),
            DMA, DMA((ney,)), DMA((ney,)),
            DMA((ney, 2)), DMA((ney, 2)), DMA((ney, 2)), DMA((ney, 2)), DMA((ney, 2)), DMA((ney, 2)),
            DMA((ney, 4)), DMA((ney, 4)),
            DMA((2, edev)), DMA((2,)), DMA((2, 2)), DMA((2,)),
            DMA((2, nex)), DMA((nj, nex)), DMA((2, ney)), DMA((nj, ney)),
        ],
        name='moe',
        compiler_params=pltpu.CompilerParams(vmem_limit_bytes=67043328, collective_id=0, has_side_effects=True),
    )(xc, h, u, back, ws1, ws3, ws2, w1, w3, w2)


def solution(mesh):
    ney, nex = mesh.shape['ey'], mesh.shape['ex']
    rows = P(('ey', 'ex'))
    rep = P()

    def local(x, kv_k, kv_v, lens, topk_idx, gates, ln1, ln2, wq, wo, ws1, ws3, ws2, w1, w3, w2):
        b = x.shape[0]
        k = topk_idx.shape[1]
        n_exp = w1.shape[0] * ney * nex
        cap = max(4, (2 * b * k + n_exp - 1) // n_exp)
        C = b
        h, u, xc, back = _attention(x, kv_k, kv_v, lens, topk_idx.T, gates.T, ln1, ln2, wq, wo, ney, n_exp, C, cap)
        return _moe(xc, h, u, back, ws1, ws3, ws2, w1, w3, w2, ney, nex, C, cap)

    return jax.shard_map(
        local, mesh=mesh,
        in_specs=(rows, rows, rows, rows, rows, rows, rep, rep, rep, rep, rep, rep, rep, rows, rows, rows),
        out_specs=rows, check_vma=False)
```
